32 devices in a mesh: batch: 16 (over z, y, x), strip: 2 (over core).
Axes of the slice: x: 2, y: 2, z: 4, core: 2. Of those that a mesh axis runs over, the one named last changes fastest.
Arguments:
- state_maps: bfloat16 [16, 32, 64, 256], P('batch', 'strip'), may hold values from -6 to 6
- goal_maps: bfloat16 [16, 32, 64, 256], P('batch', 'strip'), may hold values from -6 to 6
- conv_one: bfloat16 [3, 3, 256, 256], replicated, may hold values from -0.125 to 0.125
- conv_two: bfloat16 [3, 3, 256, 256], replicated, may hold values from -0.125 to 0.125
- state_proj: bfloat16 [256, 1024], replicated, may hold values from -0.375 to 0.375
- goal_proj: bfloat16 [256, 1024], replicated, may hold values from -0.375 to 0.375
- inv_temp: float32 [1], replicated, may hold values from 4 to 16
- pair_index: int32 [16], P('batch'), may hold values from 0 to 15, each once
Outputs:
- pair_loss: float32 [16], P('batch')
- grad_state_proj: float32 [256, 1024], replicated
- grad_goal_proj: float32 [256, 1024], replicated
- block_maps: float32 [2, 16, 32, 64, 256], P(None, 'batch', 'strip')
The draws below stay inside these ranges and needn't reach their ends.
Inputs may be any that keep to these rules, and one draw needn't show every extreme that they name: pair_index names each goal of 0 to 15 exactly once.
All inputs are finite; a program needn't handle non-finite values.
Results may differ from the reference program's by a relative error of at most 0.017.
Values may be sent and summed in bfloat16 or wider, within the bound.
A program may use at most 64 MiB of HBM per device.

```python
import jax
import jax.numpy as jnp
from jax import lax

C = 256
E = 1024
COLS = 64
ROWS = 32
PAIRS = 16


def maps_draw(base_key):
    first_key, second_key = jax.random.split(base_key, 2)
    full_shape = (PAIRS, ROWS, COLS, C)
    rough_part = jax.random.normal(first_key, full_shape, jnp.float32)
    offset = jax.random.normal(second_key, (PAIRS, 1, 1, C), jnp.float32)
    return jnp.clip(0.7 * rough_part + offset, -6.0, 6.0).astype(jnp.bfloat16)


def draw_state_maps(key, part):
    return maps_draw(jax.random.fold_in(key, 11))


def draw_goal_maps(key, part):
    return maps_draw(jax.random.fold_in(key, 23))


def centred(own_key, extent, deviation, bound, kind=jnp.bfloat16):
    return jnp.clip(deviation * jax.random.normal(own_key, extent, jnp.float32), -bound, bound).astype(kind)


def setup_inputs(seed: int = 0) -> dict:
    keys = jax.random.split(jax.random.key(seed), 9)
    return {
        "state_maps": draw_state_maps(jax.random.fold_in(keys[8], 71), 0),
        "goal_maps": draw_goal_maps(jax.random.fold_in(keys[8], 71), 0),
        "conv_one": centred(keys[2], (3, 3, C, C), (9 * C) ** -0.5, 0.125),
        "conv_two": centred(keys[3], (3, 3, C, C), (9 * C) ** -0.5, 0.125),
        "state_proj": centred(keys[4], (C, E), C ** -0.5, 0.375),
        "goal_proj": centred(keys[5], (C, E), C ** -0.5, 0.375),
        "inv_temp": jnp.clip(jax.random.uniform(keys[6], (1,), jnp.float32, 4.0, 16.0), 4.0, 16.0),
        "pair_index": jax.random.permutation(keys[7], PAIRS).astype(jnp.int32),
    }


def conv_same(frame_maps, kernel):
    return lax.conv_general_dilated(frame_maps.astype(jnp.float32), kernel.astype(jnp.float32), (1, 1), ((1, 1), (1, 1)), dimension_numbers=('NHWC', 'HWIO', 'NHWC'), precision=lax.Precision.HIGHEST)

def encode(frame_maps, conv_one, conv_two):
    active = jnp.maximum(frame_maps, 0)
    first_out = jnp.maximum(conv_same(active, conv_one), 0.0).astype(jnp.bfloat16)
    block_out = jnp.maximum(frame_maps.astype(jnp.float32) + conv_same(first_out, conv_two), 0.0)
    return (lax.optimization_barrier(jnp.mean(block_out, axis=(1, 2))), block_out)

def pooled_all(frame_maps, conv_one, conv_two):
    grouped = frame_maps.reshape((PAIRS, 1) + frame_maps.shape[1:])
    pooled, block_out = lax.map(lambda block: encode(block, conv_one, conv_two), grouped)
    return (pooled.reshape(PAIRS, C), block_out.reshape(frame_maps.shape))

def normalize(embedding):
    inverse_norm = lax.rsqrt(lax.optimization_barrier(jnp.sum(embedding * embedding, axis=-1, keepdims=True)) + 1e-06)
    return (embedding * inverse_norm, inverse_norm)

def reference(state_maps, goal_maps, conv_one, conv_two, state_proj, goal_proj, inv_temp, pair_index):
    state_pooled, state_block = pooled_all(state_maps, conv_one, conv_two)
    goal_pooled, goal_block = pooled_all(goal_maps, conv_one, conv_two)
    block_maps = jnp.stack([state_block, goal_block], axis=0)
    state_pool = state_pooled.astype(jnp.bfloat16)
    goal_pool = goal_pooled.astype(jnp.bfloat16)
    state_emb = jnp.dot(state_pool, state_proj, preferred_element_type=jnp.float32)
    goal_emb = jnp.dot(goal_pool, goal_proj, preferred_element_type=jnp.float32)
    state_unit, state_inverse = normalize(state_emb)
    goal_unit, goal_inverse = normalize(goal_emb)
    state_bf = state_unit.astype(jnp.bfloat16)
    goal_bf = goal_unit.astype(jnp.bfloat16)
    sharpness = inv_temp[0]
    logits = sharpness * jnp.dot(state_bf, goal_bf.T, preferred_element_type=jnp.float32)
    exp_logits = jnp.exp(logits)
    row_total = lax.optimization_barrier(jnp.sum(exp_logits, axis=1))
    matched = jnp.arange(PAIRS, dtype=jnp.int32)[None, :] == pair_index[:, None]
    positive = lax.optimization_barrier(jnp.sum(jnp.where(matched, logits, 0.0), axis=1))
    pair_loss = jnp.log(row_total) - positive
    logit_grad = (exp_logits / row_total[:, None] - matched.astype(jnp.float32)).astype(jnp.bfloat16)
    state_unit_grad = sharpness * jnp.dot(logit_grad, goal_bf, preferred_element_type=jnp.float32)
    goal_unit_grad = sharpness * jnp.dot(logit_grad.T, state_bf, preferred_element_type=jnp.float32)
    state_emb_grad = ((state_unit_grad - state_unit * lax.optimization_barrier(jnp.sum(state_unit * state_unit_grad, axis=-1, keepdims=True))) * state_inverse).astype(jnp.bfloat16)
    goal_emb_grad = ((goal_unit_grad - goal_unit * lax.optimization_barrier(jnp.sum(goal_unit * goal_unit_grad, axis=-1, keepdims=True))) * goal_inverse).astype(jnp.bfloat16)
    grad_state_proj = jnp.dot(state_pool.T, state_emb_grad, preferred_element_type=jnp.float32)
    grad_goal_proj = jnp.dot(goal_pool.T, goal_emb_grad, preferred_element_type=jnp.float32)
    return (pair_loss, grad_state_proj, grad_goal_proj, block_maps)
```

```python
import functools

import jax
import jax.numpy as jnp
from jax import lax
from jax.experimental import pallas as pl
from jax.experimental.pallas import tpu as pltpu
from jax.sharding import PartitionSpec as P

MESH = pl.DeviceIdType.MESH
BF = jnp.bfloat16
F32 = jnp.float32
LANES = 128


def spread(dst, frame, row, cells):
    rows, columns, channels = cells.shape
    where = lax.broadcasted_iota(jnp.int32, cells.shape, 1)
    left = jnp.where(where == 0, 0.0, pltpu.roll(cells, 1, axis=1))
    right = jnp.where(where == columns - 1, 0.0, pltpu.roll(cells, columns - 1, axis=1))
    span = pl.ds(row, rows)
    dst[frame, span, :, 0:channels] = left.astype(BF)
    dst[frame, span, :, channels : 2 * channels] = cells.astype(BF)
    dst[frame, span, :, 2 * channels : 3 * channels] = right.astype(BF)


def taps(src, frame, row, rows):
    columns, width = src.shape[2], src.shape[3]
    return jnp.concatenate(
        [src[frame, row + d : row + d + rows].reshape(rows * columns, width) for d in range(3)],
        axis=1,
    )


def block_kernel(
    batches, strips,
    state_ref, goal_ref, one_ref, two_ref, sproj_ref, gproj_ref, index_ref,
    block_ref, gathered_ref, sproj_out, gproj_out,
    maps, wide_one, wide_two, w_one, w_two, halo, part, parts, note, notes,
    load_sem, halo_send, halo_recv, part_send, part_recv, note_send, note_recv,
):
    b = lax.axis_index("batch")
    s = lax.axis_index("strip")
    rows, columns, channels = maps.shape[1], maps.shape[2], maps.shape[3]
    packs = channels // LANES

    loads = [
        pltpu.make_async_copy(state_ref.at[0], maps.at[0], load_sem.at[0]),
        pltpu.make_async_copy(one_ref, w_one, load_sem.at[1]),
        pltpu.make_async_copy(goal_ref.at[0], maps.at[1], load_sem.at[2]),
        pltpu.make_async_copy(two_ref, w_two, load_sem.at[3]),
        pltpu.make_async_copy(sproj_ref, sproj_out, load_sem.at[4]),
        pltpu.make_async_copy(gproj_ref, gproj_out, load_sem.at[5]),
    ]
    for copy in loads:
        copy.start()

    @pl.when(s == 0)
    def _():
        halo[0] = jnp.zeros(halo.shape[1:], BF)

    @pl.when(s == strips - 1)
    def _():
        halo[1] = jnp.zeros(halo.shape[1:], BF)

    barrier = pltpu.get_barrier_semaphore()

    def greet_strip(k, carry):
        pl.semaphore_signal(barrier, inc=1, device_id=(b, lax.rem(s + k, strips)), device_id_type=MESH)
        return carry

    def greet_batch(k, carry):
        pl.semaphore_signal(barrier, inc=1, device_id=(lax.rem(b + k, batches), s), device_id_type=MESH)
        return carry

    lax.fori_loop(1, batches, greet_batch, 0)
    lax.fori_loop(1, strips, greet_strip, 0)

    def first(lhs):
        return jnp.maximum(jnp.dot(lhs, w_one[...], preferred_element_type=F32), 0.0)

    def second(lhs, skip):
        return jnp.maximum(skip + jnp.dot(lhs, w_two[...], preferred_element_type=F32), 0.0)

    half = (rows - 2) // 2
    for f in range(2):
        loads[2 * f].wait()
        spread(wide_one, f, 2, jnp.maximum(maps[f].astype(F32), 0.0))
        if f == 0:
            loads[1].wait()
        for r in range(1, rows - 1, half):
            out = first(taps(wide_one, f, r + 1, half))
            spread(wide_two, f, r + 1, out.reshape(half, columns, channels))

    pl.semaphore_wait(barrier, strips + batches - 2)
    down = pltpu.make_async_remote_copy(
        src_ref=maps.at[:, rows - 2 : rows], dst_ref=halo.at[0],
        send_sem=halo_send.at[0], recv_sem=halo_recv.at[0],
        device_id=(b, lax.rem(s + 1, strips)), device_id_type=MESH,
    )
    up = pltpu.make_async_remote_copy(
        src_ref=maps.at[:, 0:2], dst_ref=halo.at[1],
        send_sem=halo_send.at[1], recv_sem=halo_recv.at[1],
        device_id=(b, lax.rem(s + strips - 1, strips)), device_id_type=MESH,
    )

    @pl.when(s < strips - 1)
    def _():
        down.start()

    @pl.when(s > 0)
    def _():
        up.start()

    loads[3].wait()
    sums = []
    half = (rows - 4) // 2
    for f in range(2):
        total = jnp.zeros((1, channels), F32)
        for r in range(2, rows - 2, half):
            skip = maps[f, r : r + half].reshape(half * columns, channels).astype(F32)
            out = second(taps(wide_two, f, r, half), skip)
            block_ref[f, 0, r : r + half] = out.reshape(half, columns, channels)
            total = total + jnp.sum(out, axis=0, keepdims=True)
        sums.append(total)

    @pl.when(s < strips - 1)
    def _():
        down.wait_send()
        up.wait_recv()

    @pl.when(s > 0)
    def _():
        up.wait_send()
        down.wait_recv()

    for f in range(2):
        spread(wide_one, f, 0, jnp.maximum(halo[0, f].astype(F32), 0.0))
        spread(wide_one, f, rows + 2, jnp.maximum(halo[1, f].astype(F32), 0.0))
    edges = [(f, r) for f in range(2) for r in (-1, rows - 1)]
    out = first(jnp.concatenate([taps(wide_one, f, r + 1, 2) for f, r in edges], axis=0))
    out = out.reshape(len(edges), 2, columns, channels)
    above = jnp.where(s > 0, 1.0, 0.0)
    below = jnp.where(s < strips - 1, 1.0, 0.0)
    for i, (f, r) in enumerate(edges):
        pair = [out[i, 0:1], out[i, 1:2]]
        if r < 0:
            pair[0] = pair[0] * above
        else:
            pair[1] = pair[1] * below
        spread(wide_two, f, r + 1, jnp.concatenate(pair, axis=0))
    edges = [(f, r) for f in range(2) for r in (0, rows - 2)]
    skip = jnp.concatenate(
        [maps[f, r : r + 2].reshape(2 * columns, channels).astype(F32) for f, r in edges], axis=0
    )
    out = second(jnp.concatenate([taps(wide_two, f, r, 2) for f, r in edges], axis=0), skip)
    for i, (f, r) in enumerate(edges):
        piece = out[2 * columns * i : 2 * columns * (i + 1)]
        block_ref[f, 0, r : r + 2] = piece.reshape(2, columns, channels)
        sums[f] = sums[f] + jnp.sum(piece, axis=0, keepdims=True)

    cells = rows * strips * columns
    lines = [total[:, LANES * p : LANES * (p + 1)] / cells for total in sums for p in range(packs)]
    blank = jnp.zeros((part.shape[0] - len(lines), LANES), F32)
    share = jnp.concatenate(lines + [blank], axis=0)
    part[...] = share
    parts[s] = share

    def part_copy(k):
        return pltpu.make_async_remote_copy(
            src_ref=part, dst_ref=parts.at[s],
            send_sem=part_send.at[k], recv_sem=part_recv.at[k],
            device_id=(b, lax.rem(s + k, strips)), device_id_type=MESH,
        )

    def note_copy(k):
        return pltpu.make_async_remote_copy(
            src_ref=note, dst_ref=notes.at[b],
            send_sem=note_send.at[k], recv_sem=note_recv.at[k],
            device_id=(lax.rem(b + k, batches), s), device_id_type=MESH,
        )

    def exchange(make, count):
        def start(k, carry):
            make(k).start()
            return carry

        def finish(k, carry):
            make(k).wait()
            return carry

        lax.fori_loop(1, count, start, 0)
        lax.fori_loop(1, count, finish, 0)

    exchange(part_copy, strips)
    pooled = jnp.sum(parts[...], axis=0)
    line = lax.broadcasted_iota(jnp.int32, pooled.shape, 0)
    pooled = jnp.where(line == 2 * packs, index_ref[0].astype(F32), pooled).astype(BF)
    note[...] = pooled
    notes[b] = pooled
    exchange(note_copy, batches)
    gathered_ref[...] = notes[...]
    loads[4].wait()
    loads[5].wait()


def unit_of(emb):
    inverse = lax.rsqrt(jnp.sum(emb * emb, axis=-1, keepdims=True) + 1e-06)
    return emb * inverse, inverse


def dot(left, right, over):
    return lax.dot_general(left, right, ((over[0:1], over[1:2]), ((), ())), preferred_element_type=F32)


def head_kernel(
    block_ref, gathered_ref, sproj_ref, gproj_ref, temp_ref,
    loss_ref, sgrad_ref, ggrad_ref, out_ref,
    sgrad, ggrad, sem,
):
    keep = pltpu.make_async_copy(block_ref, out_ref, sem.at[0])
    keep.start()
    batches = gathered_ref.shape[0]
    packs = sproj_ref.shape[0] // LANES
    heard = gathered_ref[...].astype(F32)

    def column(p):
        return jnp.concatenate([heard[i, p : p + 1] for i in range(batches)], axis=0)

    state_pool = jnp.concatenate([column(p) for p in range(packs)], axis=1).astype(BF)
    goal_pool = jnp.concatenate([column(packs + p) for p in range(packs)], axis=1).astype(BF)
    index = column(2 * packs)[:, 0:batches]
    sharpness = temp_ref[0]
    state_unit, state_inverse = unit_of(dot(state_pool, sproj_ref[...], (1, 0)))
    goal_unit, goal_inverse = unit_of(dot(goal_pool, gproj_ref[...], (1, 0)))
    state_bf = state_unit.astype(BF)
    goal_bf = goal_unit.astype(BF)
    logits = sharpness * dot(state_bf, goal_bf, (1, 1))
    exp_logits = jnp.exp(logits)
    row_total = jnp.sum(exp_logits, axis=1, keepdims=True)
    matched = lax.broadcasted_iota(jnp.int32, logits.shape, 1).astype(F32) == index
    positive = jnp.sum(jnp.where(matched, logits, 0.0), axis=1, keepdims=True)
    losses = jnp.log(row_total) - positive
    mine = lax.broadcasted_iota(jnp.int32, losses.shape, 0) == lax.axis_index("batch")
    loss_ref[0] = jnp.sum(jnp.where(mine, losses, 0.0))
    logit_grad = (exp_logits / row_total - matched.astype(F32)).astype(BF)
    copies = [keep]
    for i, (pool, unit, inverse, unit_grad, grad, target) in enumerate((
        (state_pool, state_unit, state_inverse, dot(logit_grad, goal_bf, (1, 0)), sgrad, sgrad_ref),
        (goal_pool, goal_unit, goal_inverse, dot(logit_grad, state_bf, (0, 0)), ggrad, ggrad_ref),
    )):
        unit_grad = sharpness * unit_grad
        along = jnp.sum(unit * unit_grad, axis=-1, keepdims=True)
        emb_grad = ((unit_grad - unit * along) * inverse).astype(BF)
        grad[...] = dot(pool, emb_grad, (0, 0))
        copies.append(pltpu.make_async_copy(grad, target, sem.at[1 + i]))
        copies[-1].start()
    for copy in copies:
        copy.wait()


def shards(batches, strips, state_maps, goal_maps, conv_one, conv_two, state_proj, goal_proj, inv_temp, pair_index):
    _, rows, columns, channels = state_maps.shape
    width = state_proj.shape[1]
    taps_in = conv_one.shape[0] * conv_one.shape[1] * channels
    any_spec = pl.BlockSpec(memory_space=pl.ANY)
    vmem = pl.BlockSpec(memory_space=pltpu.VMEM)
    smem = pl.BlockSpec(memory_space=pltpu.SMEM)
    block_shape = (2, 1, rows, columns, channels)
    dma = pltpu.SemaphoreType.DMA
    held = pl.pallas_call(
        functools.partial(block_kernel, batches, strips),
        out_shape=(
            pltpu.VMEM(block_shape, F32),
            pltpu.VMEM((batches, 8, LANES), BF),
            pltpu.VMEM((channels, width), BF),
            pltpu.VMEM((channels, width), BF),
        ),
        in_specs=[any_spec] * 6 + [smem],
        out_specs=(vmem, vmem, vmem, vmem),
        scratch_shapes=[
            pltpu.VMEM((2, rows, columns, channels), BF),
            pltpu.VMEM((2, rows + 4, columns, 3 * channels), BF),
            pltpu.VMEM((2, rows + 2, columns, 3 * channels), BF),
            pltpu.VMEM((taps_in, channels), BF),
            pltpu.VMEM((taps_in, channels), BF),
            pltpu.VMEM((2, 2, 2, columns, channels), BF),
            pltpu.VMEM((8, LANES), F32),
            pltpu.VMEM((strips, 8, LANES), F32),
            pltpu.VMEM((8, LANES), BF),
            pltpu.VMEM((batches, 8, LANES), BF),
            dma((6,)), dma((2,)), dma((2,)),
            dma((strips,)), dma((strips,)), dma((batches,)), dma((batches,)),
        ],
        compiler_params=pltpu.CompilerParams(
            collective_id=0, has_side_effects=True, vmem_limit_bytes=40 * 2**20
        ),
        name="block",
    )(
        state_maps, goal_maps,
        conv_one.reshape(taps_in, channels), conv_two.reshape(taps_in, channels),
        state_proj, goal_proj, pair_index,
    )
    held = [pltpu.with_memory_space_constraint(value, pltpu.VMEM) for value in held]
    return pl.pallas_call(
        head_kernel,
        out_shape=(
            jax.ShapeDtypeStruct((1,), F32),
            jax.ShapeDtypeStruct((channels, width), F32),
            jax.ShapeDtypeStruct((channels, width), F32),
            jax.ShapeDtypeStruct(block_shape, F32),
        ),
        in_specs=[vmem] * 4 + [smem],
        out_specs=(smem, any_spec, any_spec, any_spec),
        scratch_shapes=[
            pltpu.VMEM((channels, width), F32),
            pltpu.VMEM((channels, width), F32),
            dma((3,)),
        ],
        compiler_params=pltpu.CompilerParams(vmem_limit_bytes=40 * 2**20),
        name="head",
    )(*held, inv_temp)


def solution(mesh):
    placed = (
        P("batch", "strip", None, None),
        P("batch", "strip", None, None),
        P(),
        P(),
        P(),
        P(),
        P(),
        P("batch"),
    )
    return jax.shard_map(
        functools.partial(shards, mesh.shape["batch"], mesh.shape["strip"]),
        mesh=mesh,
        in_specs=placed,
        out_specs=(P("batch"), P(), P(), P(None, "batch", "strip", None, None)),
        check_vma=False,
    )
```

```python
import functools

import jax
import jax.numpy as jnp
from jax import lax
from jax.experimental import pallas as pl
from jax.experimental.pallas import tpu as pltpu
from jax.sharding import PartitionSpec as P

MESH = pl.DeviceIdType.MESH
BF = jnp.bfloat16
F32 = jnp.float32
LANES = 128


def spread(dst, frame, row, cells):
    rows, columns, channels = cells.shape
    where = lax.broadcasted_iota(jnp.int32, cells.shape, 1)
    left = jnp.where(where == 0, 0.0, pltpu.roll(cells, 1, axis=1))
    right = jnp.where(where == columns - 1, 0.0, pltpu.roll(cells, columns - 1, axis=1))
    span = pl.ds(row, rows)
    dst[frame, span, :, 0:channels] = left.astype(BF)
    dst[frame, span, :, channels : 2 * channels] = cells.astype(BF)
    dst[frame, span, :, 2 * channels : 3 * channels] = right.astype(BF)


def taps(src, frame, row, rows):
    columns, width = src.shape[2], src.shape[3]
    return jnp.concatenate(
        [src[frame, row + d : row + d + rows].reshape(rows * columns, width) for d in range(3)],
        axis=1,
    )


def block_kernel(
    batches, strips,
    state_ref, goal_ref, one_ref, two_ref, sproj_ref, gproj_ref, index_ref,
    block_ref, gathered_ref, sproj_out, gproj_out,
    maps, wide_one, wide_two, w_one, w_two, halo, part, parts, note, notes,
    load_sem, halo_send, halo_recv, part_send, part_recv, note_send, note_recv,
):
    b = lax.axis_index("batch")
    s = lax.axis_index("strip")
    rows, columns, channels = maps.shape[1], maps.shape[2], maps.shape[3]
    packs = channels // LANES

    loads = [
        pltpu.make_async_copy(state_ref.at[0], maps.at[0], load_sem.at[0]),
        pltpu.make_async_copy(one_ref, w_one, load_sem.at[1]),
        pltpu.make_async_copy(goal_ref.at[0], maps.at[1], load_sem.at[2]),
        pltpu.make_async_copy(two_ref, w_two, load_sem.at[3]),
        pltpu.make_async_copy(sproj_ref, sproj_out, load_sem.at[4]),
        pltpu.make_async_copy(gproj_ref, gproj_out, load_sem.at[5]),
    ]
    for copy in loads:
        copy.start()

    @pl.when(s == 0)
    def _():
        halo[0] = jnp.zeros(halo.shape[1:], BF)

    @pl.when(s == strips - 1)
    def _():
        halo[1] = jnp.zeros(halo.shape[1:], BF)

    barrier = pltpu.get_barrier_semaphore()

    def greet_strip(k, carry):
        pl.semaphore_signal(barrier, inc=1, device_id=(b, lax.rem(s + k, strips)), device_id_type=MESH)
        return carry

    def greet_batch(k, carry):
        pl.semaphore_signal(barrier, inc=1, device_id=(lax.rem(b + k, batches), s), device_id_type=MESH)
        return carry

    lax.fori_loop(1, batches, greet_batch, 0)
    lax.fori_loop(1, strips, greet_strip, 0)

    def first(lhs):
        return jnp.maximum(jnp.dot(lhs, w_one[...], preferred_element_type=F32), 0.0)

    def second(lhs, skip):
        return jnp.maximum(skip + jnp.dot(lhs, w_two[...], preferred_element_type=F32), 0.0)

    half = (rows - 2) // 2
    for f in range(2):
        loads[2 * f].wait()
        spread(wide_one, f, 2, jnp.maximum(maps[f].astype(F32), 0.0))
        if f == 0:
            loads[1].wait()
        for r in range(1, rows - 1, half):
            out = first(taps(wide_one, f, r + 1, half))
            spread(wide_two, f, r + 1, out.reshape(half, columns, channels))

    pl.semaphore_wait(barrier, strips + batches - 2)
    down = pltpu.make_async_remote_copy(
        src_ref=maps.at[:, rows - 2 : rows], dst_ref=halo.at[0],
        send_sem=halo_send.at[0], recv_sem=halo_recv.at[0],
        device_id=(b, lax.rem(s + 1, strips)), device_id_type=MESH,
    )
    up = pltpu.make_async_remote_copy(
        src_ref=maps.at[:, 0:2], dst_ref=halo.at[1],
        send_sem=halo_send.at[1], recv_sem=halo_recv.at[1],
        device_id=(b, lax.rem(s + strips - 1, strips)), device_id_type=MESH,
    )

    @pl.when(s < strips - 1)
    def _():
        down.start()

    @pl.when(s > 0)
    def _():
        up.start()

    loads[3].wait()
    sums = []
    half = (rows - 4) // 2
    for f in range(2):
        total = jnp.zeros((1, channels), F32)
        for r in range(2, rows - 2, half):
            skip = maps[f, r : r + half].reshape(half * columns, channels).astype(F32)
            out = second(taps(wide_two, f, r, half), skip)
            block_ref[f, 0, r : r + half] = out.reshape(half, columns, channels)
            total = total + jnp.sum(out, axis=0, keepdims=True)
        sums.append(total)

    @pl.when(s < strips - 1)
    def _():
        down.wait_send()
        up.wait_recv()

    @pl.when(s > 0)
    def _():
        up.wait_send()
        down.wait_recv()

    for f in range(2):
        spread(wide_one, f, 0, jnp.maximum(halo[0, f].astype(F32), 0.0))
        spread(wide_one, f, rows + 2, jnp.maximum(halo[1, f].astype(F32), 0.0))
    edges = [(f, r) for f in range(2) for r in (-1, rows - 1)]
    out = first(jnp.concatenate([taps(wide_one, f, r + 1, 2) for f, r in edges], axis=0))
    out = out.reshape(len(edges), 2, columns, channels)
    above = jnp.where(s > 0, 1.0, 0.0)
    below = jnp.where(s < strips - 1, 1.0, 0.0)
    for i, (f, r) in enumerate(edges):
        pair = [out[i, 0:1], out[i, 1:2]]
        if r < 0:
            pair[0] = pair[0] * above
        else:
            pair[1] = pair[1] * below
        spread(wide_two, f, r + 1, jnp.concatenate(pair, axis=0))
    edges = [(f, r) for f in range(2) for r in (0, rows - 2)]
    skip = jnp.concatenate(
        [maps[f, r : r + 2].reshape(2 * columns, channels).astype(F32) for f, r in edges], axis=0
    )
    out = second(jnp.concatenate([taps(wide_two, f, r, 2) for f, r in edges], axis=0), skip)
    for i, (f, r) in enumerate(edges):
        piece = out[2 * columns * i : 2 * columns * (i + 1)]
        block_ref[f, 0, r : r + 2] = piece.reshape(2, columns, channels)
        sums[f] = sums[f] + jnp.sum(piece, axis=0, keepdims=True)

    cells = rows * strips * columns
    lines = [total[:, LANES * p : LANES * (p + 1)] / cells for total in sums for p in range(packs)]
    blank = jnp.zeros((part.shape[0] - len(lines), LANES), F32)
    share = jnp.concatenate(lines + [blank], axis=0)
    part[...] = share
    parts[s] = share

    def part_copy(k):
        return pltpu.make_async_remote_copy(
            src_ref=part, dst_ref=parts.at[s],
            send_sem=part_send.at[k], recv_sem=part_recv.at[k],
            device_id=(b, lax.rem(s + k, strips)), device_id_type=MESH,
        )

    def note_copy(k):
        return pltpu.make_async_remote_copy(
            src_ref=note, dst_ref=notes.at[b],
            send_sem=note_send.at[k], recv_sem=note_recv.at[k],
            device_id=(lax.rem(b + k, batches), s), device_id_type=MESH,
        )

    def exchange(make, count):
        def start(k, carry):
            make(k).start()
            return carry

        def finish(k, carry):
            make(k).wait()
            return carry

        lax.fori_loop(1, count, start, 0)
        lax.fori_loop(1, count, finish, 0)

    exchange(part_copy, strips)
    pooled = jnp.sum(parts[...], axis=0)
    line = lax.broadcasted_iota(jnp.int32, pooled.shape, 0)
    pooled = jnp.where(line == 2 * packs, index_ref[0].astype(F32), pooled).astype(BF)
    note[...] = pooled
    notes[b] = pooled
    exchange(note_copy, batches)
    gathered_ref[...] = notes[...]
    loads[4].wait()
    loads[5].wait()


def unit_of(emb):
    inverse = lax.rsqrt(jnp.sum(emb * emb, axis=-1, keepdims=True) + 1e-06)
    return emb * inverse, inverse


def dot(left, right, over):
    return lax.dot_general(left, right, ((over[0:1], over[1:2]), ((), ())), preferred_element_type=F32)


def head_kernel(
    block_ref, gathered_ref, sproj_ref, gproj_ref, temp_ref,
    loss_ref, sgrad_ref, ggrad_ref, out_ref,
    sgrad, ggrad, sem,
):
    keep = pltpu.make_async_copy(block_ref, out_ref, sem.at[0])
    keep.start()
    batches = gathered_ref.shape[0]
    packs = sproj_ref.shape[0] // LANES
    heard = gathered_ref[...].astype(F32)

    def column(p):
        return jnp.concatenate([heard[i, p : p + 1] for i in range(batches)], axis=0)

    state_pool = jnp.concatenate([column(p) for p in range(packs)], axis=1).astype(BF)
    goal_pool = jnp.concatenate([column(packs + p) for p in range(packs)], axis=1).astype(BF)
    index = column(2 * packs)[:, 0:batches]
    sharpness = temp_ref[0]
    state_unit, state_inverse = unit_of(dot(state_pool, sproj_ref[...], (1, 0)))
    goal_unit, goal_inverse = unit_of(dot(goal_pool, gproj_ref[...], (1, 0)))
    state_bf = state_unit.astype(BF)
    goal_bf = goal_unit.astype(BF)
    logits = sharpness * dot(state_bf, goal_bf, (1, 1))
    exp_logits = jnp.exp(logits)
    row_total = jnp.sum(exp_logits, axis=1, keepdims=True)
    matched = lax.broadcasted_iota(jnp.int32, logits.shape, 1).astype(F32) == index
    positive = jnp.sum(jnp.where(matched, logits, 0.0), axis=1, keepdims=True)
    losses = jnp.log(row_total) - positive
    mine = lax.broadcasted_iota(jnp.int32, losses.shape, 0) == lax.axis_index("batch")
    loss_ref[0] = jnp.sum(jnp.where(mine, losses, 0.0))
    logit_grad = (exp_logits / row_total - matched.astype(F32)).astype(BF)
    copies = [keep]
    for i, (pool, unit, inverse, unit_grad, grad, target) in enumerate((
        (state_pool, state_unit, state_inverse, dot(logit_grad, goal_bf, (1, 0)), sgrad, sgrad_ref),
        (goal_pool, goal_unit, goal_inverse, dot(logit_grad, state_bf, (0, 0)), ggrad, ggrad_ref),
    )):
        unit_grad = sharpness * unit_grad
        along = jnp.sum(unit * unit_grad, axis=-1, keepdims=True)
        emb_grad = ((unit_grad - unit * along) * inverse).astype(BF)
        grad[...] = dot(pool, emb_grad, (0, 0))
        copies.append(pltpu.make_async_copy(grad, target, sem.at[1 + i]))
        copies[-1].start()
    for copy in copies:
        copy.wait()


def shards(batches, strips, state_maps, goal_maps, conv_one, conv_two, state_proj, goal_proj, inv_temp, pair_index):
    _, rows, columns, channels = state_maps.shape
    width = state_proj.shape[1]
    taps_in = conv_one.shape[0] * conv_one.shape[1] * channels
    any_spec = pl.BlockSpec(memory_space=pl.ANY)
    vmem = pl.BlockSpec(memory_space=pltpu.VMEM)
    smem = pl.BlockSpec(memory_space=pltpu.SMEM)
    block_shape = (2, 1, rows, columns, channels)
    dma = pltpu.SemaphoreType.DMA
    stay = [
        pltpu.with_memory_space_constraint(value, pltpu.HBM)
        for value in (
            state_maps, goal_maps,
            conv_one.reshape(taps_in, channels), conv_two.reshape(taps_in, channels),
            state_proj, goal_proj,
        )
    ]
    held = pl.pallas_call(
        functools.partial(block_kernel, batches, strips),
        out_shape=(
            pltpu.VMEM(block_shape, F32),
            pltpu.VMEM((batches, 8, LANES), BF),
            pltpu.VMEM((channels, width), BF),
            pltpu.VMEM((channels, width), BF),
        ),
        in_specs=[any_spec] * 6 + [smem],
        out_specs=(vmem, vmem, vmem, vmem),
        scratch_shapes=[
            pltpu.VMEM((2, rows, columns, channels), BF),
            pltpu.VMEM((2, rows + 4, columns, 3 * channels), BF),
            pltpu.VMEM((2, rows + 2, columns, 3 * channels), BF),
            pltpu.VMEM((taps_in, channels), BF),
            pltpu.VMEM((taps_in, channels), BF),
            pltpu.VMEM((2, 2, 2, columns, channels), BF),
            pltpu.VMEM((8, LANES), F32),
            pltpu.VMEM((strips, 8, LANES), F32),
            pltpu.VMEM((8, LANES), BF),
            pltpu.VMEM((batches, 8, LANES), BF),
            dma((6,)), dma((2,)), dma((2,)),
            dma((strips,)), dma((strips,)), dma((batches,)), dma((batches,)),
        ],
        compiler_params=pltpu.CompilerParams(
            collective_id=0, has_side_effects=True, vmem_limit_bytes=40 * 2**20
        ),
        name="block",
    )(*stay, pair_index)
    held = [pltpu.with_memory_space_constraint(value, pltpu.VMEM) for value in held]
    return pl.pallas_call(
        head_kernel,
        out_shape=(
            jax.ShapeDtypeStruct((1,), F32),
            jax.ShapeDtypeStruct((channels, width), F32),
            jax.ShapeDtypeStruct((channels, width), F32),
            jax.ShapeDtypeStruct(block_shape, F32),
        ),
        in_specs=[vmem] * 4 + [smem],
        out_specs=(smem, any_spec, any_spec, any_spec),
        scratch_shapes=[
            pltpu.VMEM((channels, width), F32),
            pltpu.VMEM((channels, width), F32),
            dma((3,)),
        ],
        compiler_params=pltpu.CompilerParams(vmem_limit_bytes=40 * 2**20),
        name="head",
    )(*held, inv_temp)


def solution(mesh):
    placed = (
        P("batch", "strip", None, None),
        P("batch", "strip", None, None),
        P(),
        P(),
        P(),
        P(),
        P(),
        P("batch"),
    )
    return jax.shard_map(
        functools.partial(shards, mesh.shape["batch"], mesh.shape["strip"]),
        mesh=mesh,
        in_specs=placed,
        out_specs=(P("batch"), P(), P(), P(None, "batch", "strip", None, None)),
        check_vma=False,
    )
```

```python
import functools

import jax
import jax.numpy as jnp
from jax import lax
from jax.experimental import pallas as pl
from jax.experimental.pallas import tpu as pltpu
from jax.sharding import PartitionSpec as P

MESH = pl.DeviceIdType.MESH
BF = jnp.bfloat16
F32 = jnp.float32
LANES = 128


def spread(dst, frame, row, cells):
    rows, columns, channels = cells.shape
    where = lax.broadcasted_iota(jnp.int32, cells.shape, 1)
    left = jnp.where(where == 0, 0.0, pltpu.roll(cells, 1, axis=1))
    right = jnp.where(where == columns - 1, 0.0, pltpu.roll(cells, columns - 1, axis=1))
    span = pl.ds(row, rows)
    dst[frame, span, :, 0:channels] = left.astype(BF)
    dst[frame, span, :, channels : 2 * channels] = cells.astype(BF)
    dst[frame, span, :, 2 * channels : 3 * channels] = right.astype(BF)


def taps(src, frame, row, rows):
    columns, width = src.shape[2], src.shape[3]
    return jnp.concatenate(
        [src[frame, row + d : row + d + rows].reshape(rows * columns, width) for d in range(3)],
        axis=1,
    )


def block_kernel(
    batches, strips,
    state_ref, goal_ref, one_ref, two_ref, sproj_ref, gproj_ref, index_ref,
    block_ref, gathered_ref, marks_out, sproj_out, gproj_out,
    maps, wide_one, wide_two, w_one, w_two, halo, mark, marks, part, parts, note, notes,
    load_sem, halo_send, halo_recv,
    mark_send, mark_recv, part_send, part_recv, note_send, note_recv,
):
    b = lax.axis_index("batch")
    s = lax.axis_index("strip")
    rows, columns, channels = maps.shape[1], maps.shape[2], maps.shape[3]
    packs = channels // LANES

    loads = [
        pltpu.make_async_copy(source, target, load_sem.at[i])
        for i, (source, target) in enumerate((
            (state_ref.at[0], maps.at[0]),
            (goal_ref.at[0], maps.at[1]),
            (one_ref, w_one),
            (two_ref, w_two),
            (sproj_ref, sproj_out),
            (gproj_ref, gproj_out),
        ))
    ]
    for copy in loads:
        copy.start()

    @pl.when(s == 0)
    def _():
        halo[0] = jnp.zeros(halo.shape[1:], BF)

    @pl.when(s == strips - 1)
    def _():
        halo[1] = jnp.zeros(halo.shape[1:], BF)

    mark[...] = jnp.full(mark.shape, index_ref[0].astype(F32))
    marks[b] = mark[...]
    barrier = pltpu.get_barrier_semaphore()

    def greet_strip(k, carry):
        pl.semaphore_signal(barrier, inc=1, device_id=(b, lax.rem(s + k, strips)), device_id_type=MESH)
        return carry

    def greet_batch(k, carry):
        pl.semaphore_signal(barrier, inc=1, device_id=(lax.rem(b + k, batches), s), device_id_type=MESH)
        return carry

    lax.fori_loop(1, batches, greet_batch, 0)
    lax.fori_loop(1, strips, greet_strip, 0)

    def part_copy(k):
        return pltpu.make_async_remote_copy(
            src_ref=part, dst_ref=parts.at[s],
            send_sem=part_send.at[k], recv_sem=part_recv.at[k],
            device_id=(b, lax.rem(s + k, strips)), device_id_type=MESH,
        )

    def note_copy(k):
        return pltpu.make_async_remote_copy(
            src_ref=note, dst_ref=notes.at[b],
            send_sem=note_send.at[k], recv_sem=note_recv.at[k],
            device_id=(lax.rem(b + k, batches), s), device_id_type=MESH,
        )

    def mark_copy(k):
        return pltpu.make_async_remote_copy(
            src_ref=mark, dst_ref=marks.at[b],
            send_sem=mark_send.at[k], recv_sem=mark_recv.at[k],
            device_id=(lax.rem(b + k, batches), s), device_id_type=MESH,
        )

    def start(make, count):
        def one(k, carry):
            make(k).start()
            return carry

        lax.fori_loop(1, count, one, 0)

    def finish(make, count):
        def one(k, carry):
            make(k).wait()
            return carry

        lax.fori_loop(1, count, one, 0)

    loads[0].wait()
    spread(wide_one, 0, 2, jnp.maximum(maps[0].astype(F32), 0.0))
    loads[1].wait()
    pl.semaphore_wait(barrier, strips + batches - 2)
    down = pltpu.make_async_remote_copy(
        src_ref=maps.at[:, rows - 2 : rows], dst_ref=halo.at[0],
        send_sem=halo_send.at[0], recv_sem=halo_recv.at[0],
        device_id=(b, lax.rem(s + 1, strips)), device_id_type=MESH,
    )
    up = pltpu.make_async_remote_copy(
        src_ref=maps.at[:, 0:2], dst_ref=halo.at[1],
        send_sem=halo_send.at[1], recv_sem=halo_recv.at[1],
        device_id=(b, lax.rem(s + strips - 1, strips)), device_id_type=MESH,
    )

    @pl.when(s < strips - 1)
    def _():
        down.start()

    @pl.when(s > 0)
    def _():
        up.start()

    start(mark_copy, batches)

    above = jnp.where(s > 0, 1.0, 0.0)
    below = jnp.where(s < strips - 1, 1.0, 0.0)

    def first(pieces):
        lhs = [taps(wide_one, f, r + 1, count) for f, r, count in pieces]
        lhs = lhs[0] if len(lhs) == 1 else jnp.concatenate(lhs, axis=0)
        out = jnp.maximum(jnp.dot(lhs, w_one[...], preferred_element_type=F32), 0.0)
        at = 0
        for f, r, count in pieces:
            piece = out[at : at + count * columns].reshape(count, columns, channels)
            at += count * columns
            if r < 0:
                piece = jnp.concatenate([piece[0:1] * above, piece[1:]], axis=0)
            if r + count > rows:
                piece = jnp.concatenate([piece[: count - 1], piece[count - 1 :] * below], axis=0)
            spread(wide_two, f, r + 1, piece)

    spread(wide_one, 1, 2, jnp.maximum(maps[1].astype(F32), 0.0))
    loads[2].wait()
    half = (rows - 2) // 2
    for r in range(1, rows - 1, half):
        first([(0, r, half)])

    loads[3].wait()

    @pl.when(s < strips - 1)
    def _():
        down.wait_send()
        up.wait_recv()

    @pl.when(s > 0)
    def _():
        up.wait_send()
        down.wait_recv()

    for f in range(2):
        spread(wide_one, f, 0, jnp.maximum(halo[0, f].astype(F32), 0.0))
        spread(wide_one, f, rows + 2, jnp.maximum(halo[1, f].astype(F32), 0.0))
    first([(0, -1, 2), (0, rows - 1, 2)])
    half = (rows + 2) // 2
    for r in range(-1, rows + 1, half):
        first([(1, r, half)])
    sums = []
    half = rows // 2
    for f in range(2):
        total = jnp.zeros((1, channels), F32)
        for r in range(0, rows, half):
            skip = maps[f, r : r + half].reshape(half * columns, channels).astype(F32)
            out = jnp.dot(taps(wide_two, f, r, half), w_two[...], preferred_element_type=F32)
            out = jnp.maximum(skip + out, 0.0)
            block_ref[f, 0, r : r + half] = out.reshape(half, columns, channels)
            total = total + jnp.sum(out, axis=0, keepdims=True)
        sums.append(total)

    cells = rows * strips * columns
    lines = [total[:, LANES * p : LANES * (p + 1)] / cells for total in sums for p in range(packs)]
    share = jnp.concatenate(lines, axis=0)
    part[...] = share
    parts[s] = share
    start(part_copy, strips)
    finish(part_copy, strips)
    pooled = jnp.sum(parts[...], axis=0).astype(BF)
    note[...] = pooled
    notes[b] = pooled
    start(note_copy, batches)
    finish(mark_copy, batches)
    marks_out[...] = jnp.concatenate([marks[i, 0:1] for i in range(batches)], axis=0)
    finish(note_copy, batches)
    gathered_ref[...] = notes[...]
    loads[4].wait()
    loads[5].wait()


def unit_of(emb):
    inverse = lax.rsqrt(jnp.sum(emb * emb, axis=-1, keepdims=True) + 1e-06)
    return emb * inverse, inverse


def dot(left, right, over):
    return lax.dot_general(left, right, ((over[0:1], over[1:2]), ((), ())), preferred_element_type=F32)


def head_kernel(
    block_ref, gathered_ref, marks_ref, sproj_ref, gproj_ref, temp_ref,
    loss_ref, sgrad_ref, ggrad_ref, out_ref,
    sgrad, ggrad, sem,
):
    keep = pltpu.make_async_copy(block_ref, out_ref, sem.at[0])
    keep.start()
    batches = gathered_ref.shape[0]
    packs = sproj_ref.shape[0] // LANES
    heard = gathered_ref[...].astype(F32)

    def column(p):
        return jnp.concatenate([heard[i, p : p + 1] for i in range(batches)], axis=0)

    state_pool = jnp.concatenate([column(p) for p in range(packs)], axis=1).astype(BF)
    goal_pool = jnp.concatenate([column(packs + p) for p in range(packs)], axis=1).astype(BF)
    index = marks_ref[:, 0:batches]
    sharpness = temp_ref[0]
    state_unit, state_inverse = unit_of(dot(state_pool, sproj_ref[...], (1, 0)))
    goal_unit, goal_inverse = unit_of(dot(goal_pool, gproj_ref[...], (1, 0)))
    state_bf = state_unit.astype(BF)
    goal_bf = goal_unit.astype(BF)
    logits = sharpness * dot(state_bf, goal_bf, (1, 1))
    exp_logits = jnp.exp(logits)
    row_total = jnp.sum(exp_logits, axis=1, keepdims=True)
    matched = lax.broadcasted_iota(jnp.int32, logits.shape, 1).astype(F32) == index
    positive = jnp.sum(jnp.where(matched, logits, 0.0), axis=1, keepdims=True)
    losses = jnp.log(row_total) - positive
    mine = lax.broadcasted_iota(jnp.int32, losses.shape, 0) == lax.axis_index("batch")
    loss_ref[0] = jnp.sum(jnp.where(mine, losses, 0.0))
    logit_grad = (exp_logits / row_total - matched.astype(F32)).astype(BF)
    copies = [keep]
    for i, (pool, unit, inverse, unit_grad, grad, target) in enumerate((
        (state_pool, state_unit, state_inverse, dot(logit_grad, goal_bf, (1, 0)), sgrad, sgrad_ref),
        (goal_pool, goal_unit, goal_inverse, dot(logit_grad, state_bf, (0, 0)), ggrad, ggrad_ref),
    )):
        unit_grad = sharpness * unit_grad
        along = jnp.sum(unit * unit_grad, axis=-1, keepdims=True)
        emb_grad = ((unit_grad - unit * along) * inverse).astype(BF)
        grad[...] = dot(pool, emb_grad, (0, 0))
        copies.append(pltpu.make_async_copy(grad, target, sem.at[1 + i]))
        copies[-1].start()
    for copy in copies:
        copy.wait()


def shards(batches, strips, state_maps, goal_maps, conv_one, conv_two, state_proj, goal_proj, inv_temp, pair_index):
    _, rows, columns, channels = state_maps.shape
    width = state_proj.shape[1]
    taps_in = conv_one.shape[0] * conv_one.shape[1] * channels
    any_spec = pl.BlockSpec(memory_space=pl.ANY)
    vmem = pl.BlockSpec(memory_space=pltpu.VMEM)
    smem = pl.BlockSpec(memory_space=pltpu.SMEM)
    block_shape = (2, 1, rows, columns, channels)
    dma = pltpu.SemaphoreType.DMA
    lines = 2 * channels // LANES
    stay = [
        pltpu.with_memory_space_constraint(value, pltpu.HBM)
        for value in (
            state_maps, goal_maps,
            conv_one.reshape(taps_in, channels), conv_two.reshape(taps_in, channels),
            state_proj, goal_proj,
        )
    ]
    held = pl.pallas_call(
        functools.partial(block_kernel, batches, strips),
        out_shape=(
            pltpu.VMEM(block_shape, F32),
            pltpu.VMEM((batches, lines, LANES), BF),
            pltpu.VMEM((batches, LANES), F32),
            pltpu.VMEM((channels, width), BF),
            pltpu.VMEM((channels, width), BF),
        ),
        in_specs=[any_spec] * 6 + [smem],
        out_specs=(vmem,) * 5,
        scratch_shapes=[
            pltpu.VMEM((2, rows, columns, channels), BF),
            pltpu.VMEM((2, rows + 4, columns, 3 * channels), BF),
            pltpu.VMEM((2, rows + 2, columns, 3 * channels), BF),
            pltpu.VMEM((taps_in, channels), BF),
            pltpu.VMEM((taps_in, channels), BF),
            pltpu.VMEM((2, 2, 2, columns, channels), BF),
            pltpu.VMEM((8, LANES), F32),
            pltpu.VMEM((batches, 8, LANES), F32),
            pltpu.VMEM((lines, LANES), F32),
            pltpu.VMEM((strips, lines, LANES), F32),
            pltpu.VMEM((lines, LANES), BF),
            pltpu.VMEM((batches, lines, LANES), BF),
            dma((6,)), dma((2,)), dma((2,)), dma((batches,)), dma((batches,)),
            dma((strips,)), dma((strips,)), dma((batches,)), dma((batches,)),
        ],
        compiler_params=pltpu.CompilerParams(
            collective_id=0, has_side_effects=True, vmem_limit_bytes=40 * 2**20
        ),
        name="block",
    )(*stay, pair_index)
    held = [pltpu.with_memory_space_constraint(value, pltpu.VMEM) for value in held]
    return pl.pallas_call(
        head_kernel,
        out_shape=(
            jax.ShapeDtypeStruct((1,), F32),
            jax.ShapeDtypeStruct((channels, width), F32),
            jax.ShapeDtypeStruct((channels, width), F32),
            jax.ShapeDtypeStruct(block_shape, F32),
        ),
        in_specs=[vmem] * 5 + [smem],
        out_specs=(smem, any_spec, any_spec, any_spec),
        scratch_shapes=[
            pltpu.VMEM((channels, width), F32),
            pltpu.VMEM((channels, width), F32),
            dma((3,)),
        ],
        compiler_params=pltpu.CompilerParams(vmem_limit_bytes=40 * 2**20),
        name="head",
    )(*held, inv_temp)


def solution(mesh):
    placed = (
        P("batch", "strip", None, None),
        P("batch", "strip", None, None),
        P(),
        P(),
        P(),
        P(),
        P(),
        P("batch"),
    )
    return jax.shard_map(
        functools.partial(shards, mesh.shape["batch"], mesh.shape["strip"]),
        mesh=mesh,
        in_specs=placed,
        out_specs=(P("batch"), P(), P(), P(None, "batch", "strip", None, None)),
        check_vma=False,
    )
```

```python
import functools

import jax
import jax.numpy as jnp
from jax import lax
from jax.experimental import pallas as pl
from jax.experimental.pallas import tpu as pltpu
from jax.sharding import PartitionSpec as P

MESH = pl.DeviceIdType.MESH
BF = jnp.bfloat16
F32 = jnp.float32
LANES = 128
ROWS_AT_ONCE = 6


def spread(dst, frame, row, cells):
    rows, columns, channels = cells.shape
    where = lax.broadcasted_iota(jnp.int32, cells.shape, 1)
    left = jnp.where(where == 0, 0.0, pltpu.roll(cells, 1, axis=1))
    right = jnp.where(where == columns - 1, 0.0, pltpu.roll(cells, columns - 1, axis=1))
    span = pl.ds(row, rows)
    dst[frame, span, :, 0:channels] = left.astype(BF)
    dst[frame, span, :, channels : 2 * channels] = cells.astype(BF)
    dst[frame, span, :, 2 * channels : 3 * channels] = right.astype(BF)


def chunks(start, stop):
    number = -(-(stop - start) // ROWS_AT_ONCE)
    cuts = [start + (stop - start) * i // number for i in range(number + 1)]
    return [(low, high - low) for low, high in zip(cuts, cuts[1:])]


def taps(src, frame, row, rows):
    columns, width = src.shape[2], src.shape[3]
    return jnp.concatenate(
        [src[frame, row + d : row + d + rows].reshape(rows * columns, width) for d in range(3)],
        axis=1,
    )


def block_kernel(
    batches, strips,
    state_ref, goal_ref, one_ref, two_ref, sproj_ref, gproj_ref, index_ref,
    block_ref, gathered_ref, marks_out, sproj_out, gproj_out,
    maps, wide_one, wide_two, w_one, w_two, halo, mark, marks, part, parts, note, notes,
    load_sem, halo_send, halo_recv,
    mark_send, mark_recv, part_send, part_recv, note_send, note_recv,
):
    b = lax.axis_index("batch")
    s = lax.axis_index("strip")
    rows, columns, channels = maps.shape[1], maps.shape[2], maps.shape[3]
    packs = channels // LANES

    loads = [
        pltpu.make_async_copy(source, target, load_sem.at[i])
        for i, (source, target) in enumerate((
            (state_ref.at[0], maps.at[0]),
            (goal_ref.at[0], maps.at[1]),
            (one_ref, w_one),
            (two_ref, w_two),
            (sproj_ref, sproj_out),
            (gproj_ref, gproj_out),
        ))
    ]
    for copy in loads:
        copy.start()

    @pl.when(s == 0)
    def _():
        halo[0] = jnp.zeros(halo.shape[1:], BF)

    @pl.when(s == strips - 1)
    def _():
        halo[1] = jnp.zeros(halo.shape[1:], BF)

    barrier = pltpu.get_barrier_semaphore()

    def greet_strip(k, carry):
        pl.semaphore_signal(barrier, inc=1, device_id=(b, lax.rem(s + k, strips)), device_id_type=MESH)
        return carry

    def greet_batch(k, carry):
        pl.semaphore_signal(barrier, inc=1, device_id=(lax.rem(b + k, batches), s), device_id_type=MESH)
        return carry

    lax.fori_loop(1, batches, greet_batch, 0)
    lax.fori_loop(1, strips, greet_strip, 0)

    def part_copy(k):
        return pltpu.make_async_remote_copy(
            src_ref=part, dst_ref=parts.at[s],
            send_sem=part_send.at[k], recv_sem=part_recv.at[k],
            device_id=(b, lax.rem(s + k, strips)), device_id_type=MESH,
        )

    def note_copy(k):
        return pltpu.make_async_remote_copy(
            src_ref=note, dst_ref=notes.at[b],
            send_sem=note_send.at[k], recv_sem=note_recv.at[k],
            device_id=(lax.rem(b + k, batches), s), device_id_type=MESH,
        )

    def mark_copy(k):
        return pltpu.make_async_remote_copy(
            src_ref=mark, dst_ref=marks.at[b],
            send_sem=mark_send.at[k], recv_sem=mark_recv.at[k],
            device_id=(lax.rem(b + k, batches), s), device_id_type=MESH,
        )

    def start(make, count):
        def one(k, carry):
            make(k).start()
            return carry

        lax.fori_loop(1, count, one, 0)

    def finish(make, count):
        def one(k, carry):
            make(k).wait()
            return carry

        lax.fori_loop(1, count, one, 0)

    loads[0].wait()
    spread(wide_one, 0, 2, jnp.maximum(maps[0].astype(F32), 0.0))
    told = jnp.full(mark.shape, index_ref[0].astype(F32))
    mark[...] = told
    marks[b] = told
    loads[1].wait()
    pl.semaphore_wait(barrier, strips + batches - 2)
    down = pltpu.make_async_remote_copy(
        src_ref=maps.at[:, rows - 2 : rows], dst_ref=halo.at[0],
        send_sem=halo_send.at[0], recv_sem=halo_recv.at[0],
        device_id=(b, lax.rem(s + 1, strips)), device_id_type=MESH,
    )
    up = pltpu.make_async_remote_copy(
        src_ref=maps.at[:, 0:2], dst_ref=halo.at[1],
        send_sem=halo_send.at[1], recv_sem=halo_recv.at[1],
        device_id=(b, lax.rem(s + strips - 1, strips)), device_id_type=MESH,
    )

    @pl.when(s < strips - 1)
    def _():
        down.start()

    @pl.when(s > 0)
    def _():
        up.start()

    start(mark_copy, batches)

    above = jnp.where(s > 0, 1.0, 0.0)
    below = jnp.where(s < strips - 1, 1.0, 0.0)

    def first(pieces):
        lhs = [taps(wide_one, f, r + 1, count) for f, r, count in pieces]
        lhs = lhs[0] if len(lhs) == 1 else jnp.concatenate(lhs, axis=0)
        out = jnp.maximum(jnp.dot(lhs, w_one[...], preferred_element_type=F32), 0.0)
        at = 0
        for f, r, count in pieces:
            piece = out[at : at + count * columns].reshape(count, columns, channels)
            at += count * columns
            if r < 0:
                piece = jnp.concatenate([piece[0:1] * above, piece[1:]], axis=0)
            if r + count > rows:
                piece = jnp.concatenate([piece[: count - 1], piece[count - 1 :] * below], axis=0)
            spread(wide_two, f, r + 1, piece)

    spread(wide_one, 1, 2, jnp.maximum(maps[1].astype(F32), 0.0))
    loads[2].wait()
    for r, count in chunks(1, rows - 1):
        first([(0, r, count)])

    loads[3].wait()

    @pl.when(s < strips - 1)
    def _():
        down.wait_send()
        up.wait_recv()

    @pl.when(s > 0)
    def _():
        up.wait_send()
        down.wait_recv()

    for f in range(2):
        spread(wide_one, f, 0, jnp.maximum(halo[0, f].astype(F32), 0.0))
        spread(wide_one, f, rows + 2, jnp.maximum(halo[1, f].astype(F32), 0.0))
    first([(0, -1, 2), (0, rows - 1, 2)])
    for r, count in chunks(-1, rows + 1):
        first([(1, r, count)])
    sums = []
    for f in range(2):
        total = jnp.zeros((1, channels), F32)
        for r, count in chunks(0, rows):
            skip = maps[f, r : r + count].reshape(count * columns, channels).astype(F32)
            out = jnp.dot(taps(wide_two, f, r, count), w_two[...], preferred_element_type=F32)
            out = jnp.maximum(skip + out, 0.0)
            block_ref[f, 0, r : r + count] = out.reshape(count, columns, channels)
            total = total + jnp.sum(out, axis=0, keepdims=True)
        sums.append(total)

    cells = rows * strips * columns
    lines = [total[:, LANES * p : LANES * (p + 1)] / cells for total in sums for p in range(packs)]
    share = jnp.concatenate(lines, axis=0)
    part[...] = share
    parts[s] = share
    start(part_copy, strips)
    finish(part_copy, strips)
    pooled = jnp.sum(parts[...], axis=0).astype(BF)
    note[...] = pooled
    notes[b] = pooled
    start(note_copy, batches)
    finish(mark_copy, batches)
    marks_out[...] = jnp.concatenate([marks[i, 0:1] for i in range(batches)], axis=0)
    finish(note_copy, batches)
    gathered_ref[...] = notes[...]
    loads[4].wait()
    loads[5].wait()


def unit_of(emb):
    inverse = lax.rsqrt(jnp.sum(emb * emb, axis=-1, keepdims=True) + 1e-06)
    return emb * inverse, inverse


def dot(left, right, over):
    return lax.dot_general(left, right, ((over[0:1], over[1:2]), ((), ())), preferred_element_type=F32)


def head_kernel(
    block_ref, gathered_ref, marks_ref, sproj_ref, gproj_ref, temp_ref,
    loss_ref, sgrad_ref, ggrad_ref, out_ref,
    loss, sgrad, ggrad, sem,
):
    keep = pltpu.make_async_copy(block_ref, out_ref, sem.at[0])
    keep.start()
    batches = gathered_ref.shape[0]
    packs = sproj_ref.shape[0] // LANES
    heard = gathered_ref[...].astype(F32)

    def column(p):
        return jnp.concatenate([heard[i, p : p + 1] for i in range(batches)], axis=0)

    state_pool = jnp.concatenate([column(p) for p in range(packs)], axis=1).astype(BF)
    goal_pool = jnp.concatenate([column(packs + p) for p in range(packs)], axis=1).astype(BF)
    index = marks_ref[:, 0:batches]
    sharpness = temp_ref[0]
    state_unit, state_inverse = unit_of(dot(state_pool, sproj_ref[...], (1, 0)))
    goal_unit, goal_inverse = unit_of(dot(goal_pool, gproj_ref[...], (1, 0)))
    state_bf = state_unit.astype(BF)
    goal_bf = goal_unit.astype(BF)
    logits = sharpness * dot(state_bf, goal_bf, (1, 1))
    exp_logits = jnp.exp(logits)
    row_total = jnp.sum(exp_logits, axis=1, keepdims=True)
    matched = lax.broadcasted_iota(jnp.int32, logits.shape, 1).astype(F32) == index
    positive = jnp.sum(jnp.where(matched, logits, 0.0), axis=1, keepdims=True)
    losses = jnp.log(row_total) - positive
    mine = lax.broadcasted_iota(jnp.int32, losses.shape, 0) == lax.axis_index("batch")
    loss[0] = jnp.sum(jnp.where(mine, losses, 0.0))
    say = pltpu.make_async_copy(loss, loss_ref, sem.at[1])
    say.start()
    logit_grad = (exp_logits / row_total - matched.astype(F32)).astype(BF)
    copies = [keep, say]
    for pool, unit, inverse, unit_grad, grad, target in (
        (state_pool, state_unit, state_inverse, dot(logit_grad, goal_bf, (1, 0)), sgrad, sgrad_ref),
        (goal_pool, goal_unit, goal_inverse, dot(logit_grad, state_bf, (0, 0)), ggrad, ggrad_ref),
    ):
        unit_grad = sharpness * unit_grad
        along = jnp.sum(unit * unit_grad, axis=-1, keepdims=True)
        emb_grad = ((unit_grad - unit * along) * inverse).astype(BF)
        for p in range(packs):
            span = slice(LANES * p, LANES * (p + 1))
            grad[span] = dot(pool[:, span], emb_grad, (0, 0))
            copies.append(pltpu.make_async_copy(grad.at[span], target.at[span], sem.at[len(copies)]))
            copies[-1].start()
    for copy in copies:
        copy.wait()


def shards(batches, strips, state_maps, goal_maps, conv_one, conv_two, state_proj, goal_proj, inv_temp, pair_index):
    _, rows, columns, channels = state_maps.shape
    width = state_proj.shape[1]
    taps_in = conv_one.shape[0] * conv_one.shape[1] * channels
    any_spec = pl.BlockSpec(memory_space=pl.ANY)
    smem = pl.BlockSpec(memory_space=pltpu.SMEM)
    vmem = pl.BlockSpec(memory_space=pltpu.VMEM)
    block_shape = (2, 1, rows, columns, channels)
    dma = pltpu.SemaphoreType.DMA
    lines = 2 * channels // LANES
    stay = [
        pltpu.with_memory_space_constraint(value, pltpu.HBM)
        for value in (
            state_maps, goal_maps,
            conv_one.reshape(taps_in, channels), conv_two.reshape(taps_in, channels),
            state_proj, goal_proj,
        )
    ]
    held = pl.pallas_call(
        functools.partial(block_kernel, batches, strips),
        out_shape=(
            pltpu.VMEM(block_shape, F32),
            pltpu.VMEM((batches, lines, LANES), BF),
            pltpu.VMEM((batches, LANES), F32),
            pltpu.VMEM((channels, width), BF),
            pltpu.VMEM((channels, width), BF),
        ),
        in_specs=[any_spec] * 6 + [smem],
        out_specs=(vmem,) * 5,
        scratch_shapes=[
            pltpu.VMEM((2, rows, columns, channels), BF),
            pltpu.VMEM((2, rows + 4, columns, 3 * channels), BF),
            pltpu.VMEM((2, rows + 2, columns, 3 * channels), BF),
            pltpu.VMEM((taps_in, channels), BF),
            pltpu.VMEM((taps_in, channels), BF),
            pltpu.VMEM((2, 2, 2, columns, channels), BF),
            pltpu.VMEM((8, LANES), F32),
            pltpu.VMEM((batches, 8, LANES), F32),
            pltpu.VMEM((lines, LANES), F32),
            pltpu.VMEM((strips, lines, LANES), F32),
            pltpu.VMEM((lines, LANES), BF),
            pltpu.VMEM((batches, lines, LANES), BF),
            dma((6,)), dma((2,)), dma((2,)), dma((batches,)), dma((batches,)),
            dma((strips,)), dma((strips,)), dma((batches,)), dma((batches,)),
        ],
        compiler_params=pltpu.CompilerParams(
            collective_id=0, has_side_effects=True, vmem_limit_bytes=40 * 2**20
        ),
        name="block",
    )(*stay, pair_index)
    held = [pltpu.with_memory_space_constraint(value, pltpu.VMEM) for value in held]
    return pl.pallas_call(
        head_kernel,
        out_shape=(
            jax.ShapeDtypeStruct((1,), F32),
            jax.ShapeDtypeStruct((channels, width), F32),
            jax.ShapeDtypeStruct((channels, width), F32),
            jax.ShapeDtypeStruct(block_shape, F32),
        ),
        in_specs=[vmem] * 5 + [smem],
        out_specs=(any_spec,) * 4,
        scratch_shapes=[
            pltpu.SMEM((1,), F32),
            pltpu.VMEM((channels, width), F32),
            pltpu.VMEM((channels, width), F32),
            dma((2 + 2 * (channels // LANES),)),
        ],
        compiler_params=pltpu.CompilerParams(vmem_limit_bytes=40 * 2**20),
        name="head",
    )(*held, inv_temp)


def solution(mesh):
    placed = (
        P("batch", "strip", None, None),
        P("batch", "strip", None, None),
        P(),
        P(),
        P(),
        P(),
        P(),
        P("batch"),
    )
    return jax.shard_map(
        functools.partial(shards, mesh.shape["batch"], mesh.shape["strip"]),
        mesh=mesh,
        in_specs=placed,
        out_specs=(P("batch"), P(), P(), P(None, "batch", "strip", None, None)),
        check_vma=False,
    )
```
